768 devices in a mesh: gx: 24 (over z, core), gy: 4 (over x), gz: 8 (over y).
Axes of the slice: x: 4, y: 8, z: 12, core: 2. Of those that a mesh axis runs over, the one named last changes fastest.
Arguments:
- residual: float32 [192, 32, 1024], P('gx', 'gy', 'gz'), may hold values from -18 to 18
- direction: float32 [192, 32, 1024], P('gx', 'gy', 'gz'), may hold values from -18 to 18
Outputs:
- powers: float32 [2, 4, 192, 32, 1024], P(None, None, 'gx', 'gy', 'gz')
- gram_matrix: float32 [9, 9], replicated
- projections: float32 [9], replicated
The draws below stay inside these ranges and needn't reach their ends.
All inputs are finite; a program needn't handle non-finite values.
Results may differ from the reference program's by a relative error of at most 0.00029.
Values sent between devices are 32-bit elements; how exact they have to be, the bound alone decides.
No kernel may reach another device: no remote copies, remote signals or barrier semaphores. Data moves between devices by JAX's collectives and lax.ppermute only.
A program may use at most 32 MiB of HBM per device.

```python
import jax
import jax.numpy as jnp

STEPS = 4
MARGIN = 1
SWEEPS = 3
NX = 192
NY = 32
NZ = 1024
N_GX = 24
N_GY = 4
N_GZ = 8


def cell_law(key, salt):
    shape_cells = (NX, NY, NZ)
    gaussian = jnp.clip(jax.random.normal(jax.random.fold_in(key, salt), shape_cells, jnp.float32), -4.0, 4.0)
    levels = jax.random.uniform(jax.random.fold_in(key, salt + 1), shape_cells, jnp.float32)
    spread = 0.3 * jnp.exp(levels * jnp.log(10.0))
    along_x = jnp.arange(NX, dtype=jnp.float32) / max(NX - 1, 1)
    ramped = 0.5 + along_x
    return gaussian * spread * ramped[:, None, None]


def draw_residual(key, part):
    return cell_law(key, 1)


def draw_direction(key, part):
    return cell_law(key, 5)


def setup_inputs(seed: int = 0) -> dict:
    arg_keys = jax.random.split(jax.random.key(seed), 3)
    residual = draw_residual(jax.random.fold_in(arg_keys[2], 71), 0)
    direction = draw_direction(jax.random.fold_in(arg_keys[2], 71), 0)
    return dict(residual=residual, direction=direction)


SWEEP_SCALE = 1.0 / 9.0


def grid_operator(values):
    padded = jnp.pad(values, 1)
    center = padded[1:-1, 1:-1, 1:-1]
    beside = padded[2:, 1:-1, 1:-1] + padded[:-2, 1:-1, 1:-1]
    beside = beside + padded[1:-1, 2:, 1:-1] + padded[1:-1, :-2, 1:-1]
    beside = beside + padded[1:-1, 1:-1, 2:] + padded[1:-1, 1:-1, :-2]
    return 6.0 * center - beside


def block_operator(values):
    padded = jnp.pad(values, [(0, 0), (1, 1), (0, 0), (1, 1), (0, 0), (1, 1)])
    center = padded[:, 1:-1, :, 1:-1, :, 1:-1]
    beside = padded[:, 2:, :, 1:-1, :, 1:-1] + padded[:, :-2, :, 1:-1, :, 1:-1]
    beside = beside + padded[:, 1:-1, :, 2:, :, 1:-1] + padded[:, 1:-1, :, :-2, :, 1:-1]
    beside = beside + padded[:, 1:-1, :, 1:-1, :, 2:] + padded[:, 1:-1, :, 1:-1, :, :-2]
    return 6.0 * center - beside


def extend_axis(values, position, blocks, margin):
    leading = jnp.moveaxis(values, position, 0)
    length = leading.shape[0]
    block_width = length // blocks
    trailing = leading.shape[1:]
    padded = jnp.pad(leading, [(margin, margin)] + [(0, 0)] * len(trailing))
    below_part = padded[0:length].reshape((blocks, block_width) + trailing)[:, :margin]
    middle = leading.reshape((blocks, block_width) + trailing)
    above_part = padded[2 * margin:2 * margin + length].reshape((blocks, block_width) + trailing)[:, block_width - margin:]
    joined = jnp.concatenate([below_part, middle, above_part], axis=1)
    return jnp.moveaxis(joined, (0, 1), (position, position + 1))


def fold_axis(values, position, margin):
    leading = jnp.moveaxis(values, (position, position + 1), (0, 1))
    blocks = leading.shape[0]
    block_width = leading.shape[1] - 2 * margin
    trailing = leading.shape[2:]
    length = blocks * block_width
    zero_tail = [(0, 0)] * len(trailing)
    middle = leading[:, margin:margin + block_width].reshape((length,) + trailing)
    below_part = jnp.pad(leading[:, :margin], [(0, 0), (0, block_width - margin)] + zero_tail).reshape((length,) + trailing)
    above_part = jnp.pad(leading[:, block_width + margin:], [(0, 0), (block_width - margin, 0)] + zero_tail).reshape((length,) + trailing)
    combined = jnp.pad(middle, [(margin, margin)] + zero_tail)
    combined = combined + jnp.pad(below_part, [(0, 2 * margin)] + zero_tail)
    combined = combined + jnp.pad(above_part, [(2 * margin, 0)] + zero_tail)
    return jnp.moveaxis(combined[margin:margin + length], 0, position)


def extend_grid(values):
    values = extend_axis(values, 0, N_GX, MARGIN)
    values = extend_axis(values, 2, N_GY, MARGIN)
    return extend_axis(values, 4, N_GZ, MARGIN)


def fold_grid(values):
    values = fold_axis(values, 4, MARGIN)
    values = fold_axis(values, 2, MARGIN)
    return fold_axis(values, 0, MARGIN)


def precondition(values, mask):
    source = mask * extend_grid(values)
    iterate = mask * (SWEEP_SCALE * source)
    for sweep_index in range(SWEEPS - 1):
        iterate = mask * (iterate + SWEEP_SCALE * (source - block_operator(iterate)))
    return fold_grid(iterate)


def reference(residual, direction):
    mask = extend_grid(jnp.ones(residual.shape, jnp.float32))
    cell_count = NX * NY * NZ
    p_fields = [direction]
    p_images = []
    for step_index in range(STEPS):
        p_images.append(grid_operator(p_fields[-1]))
        p_fields.append(precondition(p_images[-1], mask))
    p_images.append(grid_operator(p_fields[-1]))
    z_fields = [precondition(residual, mask)]
    z_images = []
    for step_index in range(STEPS - 1):
        z_images.append(grid_operator(z_fields[-1]))
        z_fields.append(precondition(z_images[-1], mask))
    z_images.append(grid_operator(z_fields[-1]))
    basis = p_fields + z_fields
    images = p_images + z_images
    table_rows = []
    for left_field in basis:
        table_rows.append(jnp.stack([jnp.sum(left_field * right_image) for right_image in images]))
    gram_matrix = jnp.stack(table_rows) / cell_count
    projections = jnp.stack([jnp.sum(left_field * residual) for left_field in basis]) / cell_count
    powers = jnp.stack([jnp.stack(p_fields[1:]), jnp.stack(z_fields)])
    return (powers, gram_matrix, projections)
```

```python
import jax
import jax.numpy as jnp
from jax import lax
from jax.experimental import pallas as pl
from jax.experimental.pallas import tpu as pltpu
from jax.sharding import Mesh
from jax.sharding import PartitionSpec as P

STEPS = 4
GX = ("gx_0", "gx_1")
BX, BY, BZ = 8, 8, 128
SLAB = 2 * BX
HALO = 3 * STEPS + 1
STRIP = 16
TILES = 4
ROWS = TILES * BY
PAD = 8
PLANES = SLAB + 2 * HALO
NB = 10
SHORT = HALO - BX + 2
MSG = TILES * (NB + SHORT)
C0, C1, CS = 117.0, 15.0, 1.0 / 729.0

f32 = jnp.float32


def lanes():
    return lax.broadcasted_iota(jnp.int32, (8, 128), 1)


def pack_kernel(direction, residual, up, down):
    lane = lanes()
    for k, ref in enumerate((direction, residual)):
        high = jnp.zeros((8, 128), f32)
        low = jnp.zeros((8, 128), f32)
        for p in range(BX):
            here = (lane >= STRIP * p) & (lane < STRIP * (p + 1))
            v = ref[p]
            high = jnp.where(here, pltpu.roll(v, (STRIP * p - (BZ - STRIP)) % 128, 1), high)
            low = jnp.where(here, pltpu.roll(v, STRIP * p, 1) if p else v, low)
        up[k] = high
        down[k] = low


def powers_kernel(where_ref, own, low, high, mine, theirs, images, sums, *scratch):
    fields = scratch[:5]
    flat, g0_ref, g1_ref, g2_ref, x0_ref, x1_ref, x2_ref, zw, yw = scratch[5:]
    core, ix, iy, iz = where_ref[0], where_ref[1], where_ref[2], where_ref[3]
    lane = lanes()

    one = jnp.ones((8, 128), f32)
    has_l = jnp.where(iz > 0, 1.0, 0.0).astype(f32)
    has_r = where_ref[5].astype(f32)
    first, last = lane == 0, lane == 127
    inside = [one, jnp.where(lane < STRIP, has_r, jnp.where(lane >= 128 - STRIP, has_l, 0.0))]
    for k in range(2):
        if k == 0:
            m = one + jnp.where(first, has_l, 0.0) + jnp.where(last, has_r, 0.0)
            e_left = jnp.where(first, 2.0, 1.0)
            e_right = jnp.where(last, 2.0, 1.0)
            q = jnp.where(first, 2.0 * has_l, 1.0) + jnp.where(last, 2.0 * has_r, 1.0)
        else:
            m = jnp.where(first | last, 2.0, 1.0)
            e_left = jnp.where(first, 2.0, 1.0)
            e_right = jnp.where(last, 2.0, 1.0)
            q = e_left + e_right
        zw[k, 0] = C0 * m + q
        zw[k, 1] = C1 * m
        zw[k, 2] = m
        zw[k, 3] = e_left
        zw[k, 4] = e_right
        zw[k, 5] = inside[k] * CS
        zw[k, 6] = inside[k]

    row = lax.broadcasted_iota(jnp.int32, (ROWS, 128), 0)
    top, bottom = row % BY == 0, row % BY == BY - 1
    e_up = jnp.where(top, 2.0, 1.0)
    e_down = jnp.where(bottom, 2.0, 1.0)
    yw[0] = 1.0 + jnp.where(top & (row > 0), 1.0, 0.0) + jnp.where(bottom & (row < ROWS - 1), 1.0, 0.0)
    yw[1] = e_up
    yw[2] = e_down
    yw[3] = jnp.where(row > 0, e_up, 0.0) + jnp.where(row < ROWS - 1, e_down, 0.0)

    blank = jnp.zeros((PLANES, PAD, 128), f32)
    for ref in list(fields) + [g1_ref, g2_ref]:
        for k in range(2):
            ref[k, :, 0:PAD, :] = blank
            ref[k, :, PAD + ROWS : PAD + ROWS + PAD, :] = blank

    def place(x, t, center, left, right):
        p = x % BX
        rows = slice(PAD + BY * t, PAD + BY * (t + 1))
        fields[0][0, x + HALO, rows, :] = center
        shift_r = (-STRIP * p) % 128
        shift_l = (128 - STRIP - STRIP * p) % 128
        r = pltpu.roll(right, shift_r, 1) if shift_r else right
        l = pltpu.roll(left, shift_l, 1) if shift_l else left
        fields[0][1, x + HALO, rows, :] = jnp.where(
            lane < STRIP, r, jnp.where(lane >= 128 - STRIP, l, 0.0)
        )

    for t in range(TILES):
        for c in range(2):
            left, right = own[TILES * c + t, BX], own[TILES * c + t, BX + 1]
            for p in range(BX):
                place(BX * c + p, t, own[TILES * c + t, p], left, right)
        n = SHORT - 2
        base = SHORT * t
        for p in range(n):
            place(p - HALO, t, low[base + p], low[base + n], low[base + n + 1])
        base = SHORT * TILES + NB * t
        for p in range(BX):
            place(p - BX, t, low[base + p], low[base + BX], low[base + BX + 1])
        base = NB * t
        for p in range(BX):
            place(SLAB + p, t, high[base + p], high[base + BX], high[base + BX + 1])
        base = NB * TILES + SHORT * t
        for p in range(n):
            place(SLAB + BX + p, t, high[base + p], high[base + n], high[base + n + 1])

    lane_row = lax.broadcasted_iota(jnp.int32, (ROWS, 128), 1)

    def left_of(c, s, d):
        rc, rs = pltpu.roll(c, d, 1), pltpu.roll(s, d, 1)
        edge = lane_row < d
        return jnp.where(edge, rs, rc), jnp.where(edge, rc, rs)

    def right_of(c, s, d):
        rc, rs = pltpu.roll(c, 128 - d, 1), pltpu.roll(s, 128 - d, 1)
        edge = lane_row >= 128 - d
        return jnp.where(edge, rs, rc), jnp.where(edge, rc, rs)

    n_planes = where_ref[4]

    def in_grid(i):
        g = ix * SLAB + i - HALO
        return jnp.where((g >= 0) & (g < n_planes), 1.0, 0.0).astype(f32)

    def z_row(k, j):
        return zw[k, j][0:1, :]

    def around(ref, i):
        c, s = ref[0, i, PAD : PAD + ROWS, :], ref[1, i, PAD : PAD + ROWS, :]
        lc, ls = left_of(c, s, 1)
        rc, rs = right_of(c, s, 1)
        out = []
        for k, (v, a, b) in enumerate(((c, lc, rc), (s, ls, rs))):
            n = a + b
            n = n + (ref[k, i, PAD - 1 : PAD - 1 + ROWS, :] + ref[k, i, PAD + 1 : PAD + 1 + ROWS, :])
            n = n + (ref[k, i - 1, PAD : PAD + ROWS, :] + ref[k, i + 1, PAD : PAD + ROWS, :])
            out.append((v, n))
        return out

    for step in range(STEPS):
        source, target = fields[step], fields[step + 1]
        lo_b = 1 + 3 * step
        hi_b = PLANES - 1 - 3 * step

        def image_and_z(i, _, step=step, source=source):
            (c, nc), (s, ns) = around(source, i)
            if step == 0:
                center = jnp.where(core == 0, 6.0, 1.0).astype(f32)
                beside = jnp.where(core == 0, 1.0, 0.0).astype(f32)
                ac, as_ = center * c - beside * nc, center * s - beside * ns
            else:
                ac, as_ = 6.0 * c - nc, 6.0 * s - ns
            flat[step, i] = ac
            keep = in_grid(i)
            bc, bs = ac * (z_row(0, 5) * keep), as_ * (z_row(1, 5) * keep)
            l1c, l1s = left_of(bc, bs, 1)
            r1c, r1s = right_of(bc, bs, 1)
            l2c, l2s = left_of(bc, bs, 2)
            r2c, r2s = right_of(bc, bs, 2)
            for k, (b, l1, r1, l2, r2) in enumerate(((bc, l1c, r1c, l2c, r2c), (bs, l1s, r1s, l2s, r2s))):
                e = z_row(k, 3) * l1 + z_row(k, 4) * r1
                g0_ref[k, i] = z_row(k, 0) * b + C1 * e + (l2 + r2)
                g1_ref[k, i, PAD : PAD + ROWS, :] = z_row(k, 1) * b + (e + e)
                g2_ref[k, i, PAD : PAD + ROWS, :] = z_row(k, 2) * b
            return 0

        lax.fori_loop(lo_b, hi_b, image_and_z, 0)

        def along_y(i, _):
            for k in range(2):
                g1 = g1_ref[k, i, PAD : PAD + ROWS, :]
                g2 = g2_ref[k, i, PAD : PAD + ROWS, :]
                m, up, down, q = yw[0], yw[1], yw[2], yw[3]
                e1 = up * g1_ref[k, i, PAD - 1 : PAD - 1 + ROWS, :] + down * g1_ref[k, i, PAD + 1 : PAD + 1 + ROWS, :]
                e2 = up * g2_ref[k, i, PAD - 1 : PAD - 1 + ROWS, :] + down * g2_ref[k, i, PAD + 1 : PAD + 1 + ROWS, :]
                far = g2_ref[k, i, PAD - 2 : PAD - 2 + ROWS, :] + g2_ref[k, i, PAD + 2 : PAD + 2 + ROWS, :]
                x0_ref[k, i] = m * g0_ref[k, i] + e1 + (q * g2 + far)
                x1_ref[k, i] = m * g1 + (e2 + e2)
                x2_ref[k, i] = m * g2
            return 0

        lax.fori_loop(lo_b, hi_b, along_y, 0)

        def along_x(i, _, target=target):
            g = ix * SLAB + i - HALO
            keep = in_grid(i)
            p = g & (BX - 1)
            before = jnp.where(p == 0, 2.0, 1.0).astype(f32)
            after = jnp.where(p == BX - 1, 2.0, 1.0).astype(f32)
            some_before = jnp.where(g > 0, 1.0, 0.0).astype(f32)
            some_after = jnp.where(g < n_planes - 1, 1.0, 0.0).astype(f32)
            m = keep * (1.0 + (before - 1.0) * some_before + (after - 1.0) * some_after)
            q = keep * (before * some_before + after * some_after)
            wl, wr = keep * before, keep * after
            for k in range(2):
                v = m * x0_ref[k, i] + q * x2_ref[k, i]
                v = v + (wl * x1_ref[k, i - 1] + wr * x1_ref[k, i + 1])
                v = v + keep * (x2_ref[k, i - 2] + x2_ref[k, i + 2])
                if k == 1:
                    v = v * z_row(1, 6)
                target[k, i, PAD : PAD + ROWS, :] = v
            return 0

        lax.fori_loop(lo_b + 2, hi_b - 2, along_x, 0)

    def last_image(i, _):
        c, nc = around(fields[STEPS], i)[0]
        flat[STEPS, i] = 6.0 * c - nc
        return 0

    lax.fori_loop(HALO, HALO + SLAB, last_image, 0)

    rows = pl.ds(pl.multiple_of(PAD + BY * iy, 8), BY)
    flat_rows = pl.ds(pl.multiple_of(BY * iy, 8), BY)
    for j in range(1, STEPS + 1):
        mine[j - 1] = fields[j][0, pl.ds(HALO + BX * core, BX), rows, :]
        theirs[j - 1] = fields[j][0, pl.ds(HALO + BX * (1 - core), BX), rows, :]
    for j in range(STEPS + 1):
        images[j] = flat[j, pl.ds(HALO + BX * core, BX), flat_rows, :]
        theirs[STEPS + j] = flat[j, pl.ds(HALO + BX * (1 - core), BX), flat_rows, :]

    pairs = [(a, b) for a in range(STEPS + 1) for b in range(a, STEPS + 1)]
    totals = [jnp.zeros((8, 128), f32) for _ in pairs]
    for x in range(SLAB):
        fs = [fields[j][0, HALO + x, rows, :] for j in range(STEPS + 1)]
        im = [flat[j, HALO + x, flat_rows, :] for j in range(STEPS + 1)]
        totals = [total + fs[a] * im[b] for total, (a, b) in zip(totals, pairs)]
    sums[...] = jnp.zeros((16, 128), f32)
    for n, total in enumerate(totals):
        sums[n : n + 1, :] = jnp.sum(total, axis=0, keepdims=True)


def products_kernel(where_ref, mine, other, images, sums, direction, residual, powers, row, table):
    north = where_ref[0] == 0
    d, r = direction[...], residual[...]
    own = [jnp.where(north, d, r)] + [mine[j] for j in range(STEPS)]
    far = [jnp.where(north, r, d)] + [other[j] for j in range(STEPS)]
    p = [d] + [jnp.where(north, own[j], far[j]) for j in range(1, STEPS + 1)]
    z = [jnp.where(north, far[j], own[j]) for j in range(1, STEPS + 1)]
    for j in range(STEPS):
        powers[0, j] = p[j + 1]
        powers[1, j] = z[j]

    def fold(v):
        return jnp.sum(jnp.sum(v, axis=0), axis=0, keepdims=True)

    zero = jnp.zeros((1, 128), f32)
    local = {}
    n = 0
    for a in range(STEPS + 1):
        for b in range(a, STEPS + 1):
            local[a, b] = local[b, a] = sums[n : n + 1, :]
            n += 1
    image = [jnp.where(north, images[a], other[STEPS + a]) for a in range(STEPS + 1)]
    cross = [[fold(image[a] * z[b]) for b in range(STEPS)] for a in range(STEPS + 1)]
    table[...] = jnp.zeros((128, 128), f32)
    size = 2 * STEPS + 1
    for a in range(size):
        for b in range(size):
            if a <= STEPS and b <= STEPS:
                v = jnp.where(north, local[a, b], zero)
            elif a > STEPS and b > STEPS:
                v = jnp.where(north, zero, local[a - STEPS, b - STEPS])
            else:
                v = cross[min(a, b)][max(a, b) - STEPS - 1]
            table[size * a + b : size * a + b + 1, :] = v
    for a, v in enumerate(p + z):
        at = size * size + a
        table[at : at + 1, :] = fold(v * r)
    row[...] = lax.dot_general(
        jnp.ones((8, 128), f32),
        table[...],
        (((1,), (1,)), ((), ())),
        precision=lax.Precision.HIGHEST,
        preferred_element_type=f32,
    )[0:1, :]


def total_kernel(parts, gram, projections, *, scale):
    size = 2 * STEPS + 1
    total = parts[0]
    for n in range(1, parts.shape[0]):
        total = total + parts[n]
    total = total * scale
    wide = jnp.broadcast_to(total, (8, 128))
    for a in range(size):
        v = pltpu.roll(wide, (128 - size * a) % 128, 1) if a else wide
        gram[a : a + 1, :] = v[0:1, 0:size]
    v = pltpu.roll(wide, (128 - size * size) % 128, 1)
    projections[...] = v[0:1, 0:size]


VMEM = pl.BlockSpec(memory_space=pltpu.VMEM)
SMEM = pl.BlockSpec(memory_space=pltpu.SMEM)


def shaped(*dims):
    return jax.ShapeDtypeStruct(dims, f32)


def pack(direction, residual):
    return pl.pallas_call(
        pack_kernel,
        in_specs=[VMEM, VMEM],
        out_specs=[VMEM, VMEM],
        out_shape=[shaped(2, 8, 128), shaped(2, 8, 128)],
        name="pack",
    )(direction, residual)


def powers_of(where, own, low, high, interpret=False):
    padded = (2, PLANES, ROWS + 2 * PAD, 128)
    plain = (2, PLANES, ROWS, 128)
    return pl.pallas_call(
        powers_kernel,
        in_specs=[SMEM, VMEM, VMEM, VMEM],
        out_specs=[VMEM] * 4,
        out_shape=[
            shaped(STEPS, 8, 8, 128),
            shaped(2 * STEPS + 1, 8, 8, 128),
            shaped(STEPS + 1, 8, 8, 128),
            shaped(16, 128),
        ],
        scratch_shapes=[pltpu.VMEM(padded, f32)] * 5
        + [pltpu.VMEM((STEPS + 1, PLANES, ROWS, 128), f32)]
        + [pltpu.VMEM(plain, f32), pltpu.VMEM(padded, f32), pltpu.VMEM(padded, f32)]
        + [pltpu.VMEM(plain, f32)] * 3
        + [pltpu.VMEM((2, 7, 8, 128), f32), pltpu.VMEM((4, ROWS, 128), f32)],
        compiler_params=pltpu.CompilerParams(vmem_limit_bytes=48 * 1024 * 1024),
        interpret=interpret,
        name="powers",
    )(where, own, low, high)


def products(where, mine, other, images, sums, direction, residual, interpret=False):
    return pl.pallas_call(
        products_kernel,
        in_specs=[SMEM] + [VMEM] * 6,
        out_specs=[VMEM, VMEM],
        out_shape=[shaped(2, STEPS, 8, 8, 128), shaped(1, 128)],
        scratch_shapes=[pltpu.VMEM((128, 128), f32)],
        interpret=interpret,
        name="products",
    )(where, mine, other, images, sums, direction, residual)


def totals(parts, scale, interpret=False):
    size = 2 * STEPS + 1

    def kernel(parts_ref, gram, projections):
        total_kernel(parts_ref, gram, projections, scale=scale)

    return pl.pallas_call(
        kernel,
        in_specs=[VMEM],
        out_specs=[VMEM, VMEM],
        out_shape=[shaped(size, size), shaped(1, size)],
        interpret=interpret,
        name="totals",
    )(parts)


def block_message(cells, left, right):
    return jnp.concatenate([cells, left[None], right[None]], axis=0)


def x_messages(own):
    n = SHORT - 2
    first, second = own[:TILES], own[TILES:]
    flat = lambda v: v.reshape(-1, 8, 128)
    up = jnp.concatenate([flat(first[:, BX - n :]), flat(second)], axis=0)
    short = jnp.concatenate([second[:, :n], second[:, BX:]], axis=1)
    down = jnp.concatenate([flat(first), flat(short)], axis=0)
    return up, down


def forward(n):
    return [(i, i + 1) for i in range(n - 1)]


def backward(n):
    return [(i + 1, i) for i in range(n - 1)]


def everyone(x, axes, count):
    return lax.all_to_all(jnp.broadcast_to(x[None], (count,) + x.shape), axes, 0, 0)


def local(residual, direction):
    nx, ny, nz = lax.axis_size("gx_0"), lax.axis_size("gy"), lax.axis_size("gz")
    iz = lax.axis_index("gz")
    where = jnp.stack(
        [
            lax.axis_index("gx_1"),
            lax.axis_index("gx_0"),
            lax.axis_index("gy"),
            iz,
            jnp.int32(nx * SLAB),
            jnp.where(iz < nz - 1, 1, 0),
        ]
    ).astype(jnp.int32)
    up, down = pack(direction, residual)
    left = lax.ppermute(up, "gz", forward(nz))
    right = lax.ppermute(down, "gz", backward(nz))
    message = jnp.stack(
        [block_message(direction, left[0], right[0]), block_message(residual, left[1], right[1])]
    )
    message = jnp.broadcast_to(message[:, None], (2, TILES) + message.shape[1:])
    own = lax.all_to_all(message.reshape((2 * TILES,) + message.shape[2:]), ("gx_1", "gy"), 0, 0)
    send_up, send_down = x_messages(own)
    low = lax.ppermute(send_up, "gx_0", forward(nx))
    high = lax.ppermute(send_down, "gx_0", backward(nx))
    mine, theirs, images, sums = powers_of(where, own, low, high)
    other = lax.ppermute(theirs, "gx_1", [(0, 1), (1, 0)])
    powers, row = products(where, mine, other, images, sums, direction, residual)
    row = jnp.sum(everyone(row, ("gy", "gz"), ny * nz), axis=0)
    parts = everyone(row, GX, 2 * nx)
    cells = float(2 * nx * BX * ny * BY * nz * BZ)
    gram, projections = totals(parts, 1.0 / cells)
    return powers, gram, projections.reshape(-1)


def solution(mesh):
    torus = Mesh(
        mesh.devices.reshape(mesh.shape["gx"] // 2, 2, mesh.shape["gy"], mesh.shape["gz"]),
        ("gx_0", "gx_1", "gy", "gz"),
    )
    return jax.shard_map(
        local,
        mesh=torus,
        in_specs=(P(GX, "gy", "gz"), P(GX, "gy", "gz")),
        out_specs=(P(None, None, GX, "gy", "gz"), P(), P()),
        check_vma=False,
    )
```

```python
import jax
import jax.numpy as jnp
from jax import lax
from jax.experimental import pallas as pl
from jax.experimental.pallas import tpu as pltpu
from jax.sharding import Mesh
from jax.sharding import PartitionSpec as P

STEPS = 4
GX = ("gx_0", "gx_1")
BX, BY, BZ = 8, 8, 128
SLAB = 2 * BX
HALO = 3 * STEPS + 1
STRIP = 16
TILES = 4
ROWS = TILES * BY
PAD = 8
PLANES = SLAB + 2 * HALO
NB = 10
SHORT = HALO - BX + 2
MSG = TILES * (NB + SHORT)
UNROLL = 4
LEAD = UNROLL + 6
ORIGIN = LEAD + HALO
C0, C1, CS = 117.0, 15.0, 1.0 / 729.0

f32 = jnp.float32


def lanes():
    return lax.broadcasted_iota(jnp.int32, (8, 128), 1)


def pack_kernel(direction, residual, up, down):
    lane = lanes()
    for k, ref in enumerate((direction, residual)):
        high = jnp.zeros((8, 128), f32)
        low = jnp.zeros((8, 128), f32)
        for p in range(BX):
            here = (lane >= STRIP * p) & (lane < STRIP * (p + 1))
            v = ref[p]
            high = jnp.where(here, pltpu.roll(v, (STRIP * p - (BZ - STRIP)) % 128, 1), high)
            low = jnp.where(here, pltpu.roll(v, STRIP * p, 1) if p else v, low)
        up[k] = high
        down[k] = low


def powers_kernel(where_ref, own, low, high, mine, theirs, images, sums, *scratch):
    fields = scratch[:5]
    flat, b_ref, g0_ref, g1_ref, g2_ref, x0_ref, x1_ref, x2_ref, zw, yw = scratch[5:]
    core, ix, iy, iz = where_ref[0], where_ref[1], where_ref[2], where_ref[3]
    lane = lanes()

    one = jnp.ones((8, 128), f32)
    has_l = jnp.where(iz > 0, 1.0, 0.0).astype(f32)
    has_r = where_ref[5].astype(f32)
    first, last = lane == 0, lane == 127
    inside = [one, jnp.where(lane < STRIP, has_r, jnp.where(lane >= 128 - STRIP, has_l, 0.0))]
    for k in range(2):
        if k == 0:
            m = one + jnp.where(first, has_l, 0.0) + jnp.where(last, has_r, 0.0)
            e_left = jnp.where(first, 2.0, 1.0)
            e_right = jnp.where(last, 2.0, 1.0)
            q = jnp.where(first, 2.0 * has_l, 1.0) + jnp.where(last, 2.0 * has_r, 1.0)
        else:
            m = jnp.where(first | last, 2.0, 1.0)
            e_left = jnp.where(first, 2.0, 1.0)
            e_right = jnp.where(last, 2.0, 1.0)
            q = e_left + e_right
        zw[k, 0] = C0 * m + q
        zw[k, 1] = C1 * m
        zw[k, 2] = m
        zw[k, 3] = e_left
        zw[k, 4] = e_right
        zw[k, 5] = inside[k] * CS
        zw[k, 6] = inside[k]

    row = lax.broadcasted_iota(jnp.int32, (ROWS, 128), 0)
    top, bottom = row % BY == 0, row % BY == BY - 1
    e_up = jnp.where(top, 2.0, 1.0)
    e_down = jnp.where(bottom, 2.0, 1.0)
    yw[0] = 1.0 + jnp.where(top & (row > 0), 1.0, 0.0) + jnp.where(bottom & (row < ROWS - 1), 1.0, 0.0)
    yw[1] = e_up
    yw[2] = e_down
    yw[3] = jnp.where(row > 0, e_up, 0.0) + jnp.where(row < ROWS - 1, e_down, 0.0)

    blank = jnp.zeros((PAD, 128), f32)

    def clear(i, _):
        for ref in list(fields) + [g1_ref, g2_ref]:
            for k in range(2):
                ref[k, i, 0:PAD, :] = blank
                ref[k, i, PAD + ROWS : PAD + ROWS + PAD, :] = blank
        return 0

    lax.fori_loop(LEAD, LEAD + PLANES, clear, 0)

    def place(x, t, center, left, right):
        p = x % BX
        rows = slice(PAD + BY * t, PAD + BY * (t + 1))
        fields[0][0, x + ORIGIN, rows, :] = center
        shift_r = (-STRIP * p) % 128
        shift_l = (128 - STRIP - STRIP * p) % 128
        r = pltpu.roll(right, shift_r, 1) if shift_r else right
        l = pltpu.roll(left, shift_l, 1) if shift_l else left
        fields[0][1, x + ORIGIN, rows, :] = jnp.where(
            lane < STRIP, r, jnp.where(lane >= 128 - STRIP, l, 0.0)
        )

    for t in range(TILES):
        for c in range(2):
            left, right = own[TILES * c + t, BX], own[TILES * c + t, BX + 1]
            for p in range(BX):
                place(BX * c + p, t, own[TILES * c + t, p], left, right)
        n = SHORT - 2
        base = SHORT * t
        for p in range(n):
            place(p - HALO, t, low[base + p], low[base + n], low[base + n + 1])
        base = SHORT * TILES + NB * t
        for p in range(BX):
            place(p - BX, t, low[base + p], low[base + BX], low[base + BX + 1])
        base = NB * t
        for p in range(BX):
            place(SLAB + p, t, high[base + p], high[base + BX], high[base + BX + 1])
        base = NB * TILES + SHORT * t
        for p in range(n):
            place(SLAB + BX + p, t, high[base + p], high[base + n], high[base + n + 1])

    lane_row = lax.broadcasted_iota(jnp.int32, (ROWS, 128), 1)

    def left_of(c, s, d):
        rc, rs = pltpu.roll(c, d, 1), pltpu.roll(s, d, 1)
        edge = lane_row < d
        return jnp.where(edge, rs, rc), jnp.where(edge, rc, rs)

    def right_of(c, s, d):
        rc, rs = pltpu.roll(c, 128 - d, 1), pltpu.roll(s, 128 - d, 1)
        edge = lane_row >= 128 - d
        return jnp.where(edge, rs, rc), jnp.where(edge, rc, rs)

    n_planes = where_ref[4]

    def in_grid(i):
        g = ix * SLAB + i - ORIGIN
        return jnp.where((g >= 0) & (g < n_planes), 1.0, 0.0).astype(f32)

    def z_row(k, j):
        return zw[k, j][0:1, :]

    def around(ref, i):
        c, s = ref[0, i, PAD : PAD + ROWS, :], ref[1, i, PAD : PAD + ROWS, :]
        lc, ls = left_of(c, s, 1)
        rc, rs = right_of(c, s, 1)
        out = []
        for k, (v, a, b) in enumerate(((c, lc, rc), (s, ls, rs))):
            n = a + b
            n = n + (ref[k, i, PAD - 1 : PAD - 1 + ROWS, :] + ref[k, i, PAD + 1 : PAD + 1 + ROWS, :])
            n = n + (ref[k, i - 1, PAD : PAD + ROWS, :] + ref[k, i + 1, PAD : PAD + ROWS, :])
            out.append((v, n))
        return out

    for step in range(STEPS):
        source, target = fields[step], fields[step + 1]
        lo_b = LEAD + 1 + 3 * step
        hi_b = LEAD + PLANES - 1 - 3 * step

        def image(i, step=step, source=source):
            (c, nc), (s, ns) = around(source, i)
            if step == 0:
                center = jnp.where(core == 0, 6.0, 1.0).astype(f32)
                beside = jnp.where(core == 0, 1.0, 0.0).astype(f32)
                ac, as_ = center * c - beside * nc, center * s - beside * ns
            else:
                ac, as_ = 6.0 * c - nc, 6.0 * s - ns
            flat[step, i] = ac
            keep = in_grid(i)
            b_ref[0, i] = ac * (z_row(0, 5) * keep)
            b_ref[1, i] = as_ * (z_row(1, 5) * keep)

        def along_z(i):
            bc, bs = b_ref[0, i], b_ref[1, i]
            l1c, l1s = left_of(bc, bs, 1)
            r1c, r1s = right_of(bc, bs, 1)
            l2c, l2s = left_of(bc, bs, 2)
            r2c, r2s = right_of(bc, bs, 2)
            for k, (b, l1, r1, l2, r2) in enumerate(((bc, l1c, r1c, l2c, r2c), (bs, l1s, r1s, l2s, r2s))):
                e = z_row(k, 3) * l1 + z_row(k, 4) * r1
                g0_ref[k, i] = z_row(k, 0) * b + C1 * e + (l2 + r2)
                g1_ref[k, i, PAD : PAD + ROWS, :] = z_row(k, 1) * b + (e + e)
                g2_ref[k, i, PAD : PAD + ROWS, :] = z_row(k, 2) * b


        def along_y(i):
            for k in range(2):
                g1 = g1_ref[k, i, PAD : PAD + ROWS, :]
                g2 = g2_ref[k, i, PAD : PAD + ROWS, :]
                m, up, down, q = yw[0], yw[1], yw[2], yw[3]
                e1 = up * g1_ref[k, i, PAD - 1 : PAD - 1 + ROWS, :] + down * g1_ref[k, i, PAD + 1 : PAD + 1 + ROWS, :]
                e2 = up * g2_ref[k, i, PAD - 1 : PAD - 1 + ROWS, :] + down * g2_ref[k, i, PAD + 1 : PAD + 1 + ROWS, :]
                far = g2_ref[k, i, PAD - 2 : PAD - 2 + ROWS, :] + g2_ref[k, i, PAD + 2 : PAD + 2 + ROWS, :]
                x0_ref[k, i] = m * g0_ref[k, i] + e1 + (q * g2 + far)
                x1_ref[k, i] = m * g1 + (e2 + e2)
                x2_ref[k, i] = m * g2


        def along_x(i, target=target):
            g = ix * SLAB + i - ORIGIN
            keep = in_grid(i)
            p = g & (BX - 1)
            before = jnp.where(p == 0, 2.0, 1.0).astype(f32)
            after = jnp.where(p == BX - 1, 2.0, 1.0).astype(f32)
            some_before = jnp.where(g > 0, 1.0, 0.0).astype(f32)
            some_after = jnp.where(g < n_planes - 1, 1.0, 0.0).astype(f32)
            m = keep * (1.0 + (before - 1.0) * some_before + (after - 1.0) * some_after)
            q = keep * (before * some_before + after * some_after)
            wl, wr = keep * before, keep * after
            for k in range(2):
                v = m * x0_ref[k, i] + q * x2_ref[k, i]
                v = v + (wl * x1_ref[k, i - 1] + wr * x1_ref[k, i + 1])
                v = v + keep * (x2_ref[k, i - 2] + x2_ref[k, i + 2])
                if k == 1:
                    v = v * z_row(1, 6)
                target[k, i, PAD : PAD + ROWS, :] = v

        def turn(n, _, lo_b=lo_b):
            i = lo_b + UNROLL * n
            for u in range(UNROLL):
                along_z(i + u - UNROLL)
            for u in range(UNROLL):
                along_y(i + u - UNROLL)
            for u in range(UNROLL):
                along_x(i + u - UNROLL - 2)
            for u in range(UNROLL):
                image(i + u)
            return 0

        lax.fori_loop(0, -(-(hi_b - lo_b) // UNROLL) + 1, turn, 0)

    def last_image(i):
        c, nc = around(fields[STEPS], i)[0]
        flat[STEPS, i] = 6.0 * c - nc

    def last_turn(n, _):
        for u in range(SLAB // 2):
            last_image(ORIGIN + SLAB // 2 * n + u)
        return 0

    lax.fori_loop(0, 2, last_turn, 0)

    rows = pl.ds(pl.multiple_of(PAD + BY * iy, 8), BY)
    flat_rows = pl.ds(pl.multiple_of(BY * iy, 8), BY)
    for j in range(1, STEPS + 1):
        mine[j - 1] = fields[j][0, pl.ds(ORIGIN + BX * core, BX), rows, :]
        theirs[j - 1] = fields[j][0, pl.ds(ORIGIN + BX * (1 - core), BX), rows, :]
    for j in range(STEPS + 1):
        images[j] = flat[j, pl.ds(ORIGIN + BX * core, BX), flat_rows, :]
        theirs[STEPS + j] = flat[j, pl.ds(ORIGIN + BX * (1 - core), BX), flat_rows, :]

    pairs = [(a, b) for a in range(STEPS + 1) for b in range(a, STEPS + 1)]
    totals = [jnp.zeros((8, 128), f32) for _ in pairs]
    for x in range(SLAB):
        fs = [fields[j][0, ORIGIN + x, rows, :] for j in range(STEPS + 1)]
        im = [flat[j, ORIGIN + x, flat_rows, :] for j in range(STEPS + 1)]
        totals = [total + fs[a] * im[b] for total, (a, b) in zip(totals, pairs)]
    sums[...] = jnp.zeros((16, 128), f32)
    for n, total in enumerate(totals):
        sums[n : n + 1, :] = jnp.sum(total, axis=0, keepdims=True)


def products_kernel(where_ref, mine, other, images, sums, direction, residual, powers, row, table):
    north = where_ref[0] == 0
    d, r = direction[...], residual[...]
    own = [jnp.where(north, d, r)] + [mine[j] for j in range(STEPS)]
    far = [jnp.where(north, r, d)] + [other[j] for j in range(STEPS)]
    p = [d] + [jnp.where(north, own[j], far[j]) for j in range(1, STEPS + 1)]
    z = [jnp.where(north, far[j], own[j]) for j in range(1, STEPS + 1)]
    for j in range(STEPS):
        powers[0, j] = p[j + 1]
        powers[1, j] = z[j]

    def fold(v):
        return jnp.sum(jnp.sum(v, axis=0), axis=0, keepdims=True)

    zero = jnp.zeros((1, 128), f32)
    local = {}
    n = 0
    for a in range(STEPS + 1):
        for b in range(a, STEPS + 1):
            local[a, b] = local[b, a] = sums[n : n + 1, :]
            n += 1
    image = [jnp.where(north, images[a], other[STEPS + a]) for a in range(STEPS + 1)]
    cross = [[fold(image[a] * z[b]) for b in range(STEPS)] for a in range(STEPS + 1)]
    table[...] = jnp.zeros((128, 128), f32)
    size = 2 * STEPS + 1
    for a in range(size):
        for b in range(size):
            if a <= STEPS and b <= STEPS:
                v = jnp.where(north, local[a, b], zero)
            elif a > STEPS and b > STEPS:
                v = jnp.where(north, zero, local[a - STEPS, b - STEPS])
            else:
                v = cross[min(a, b)][max(a, b) - STEPS - 1]
            table[size * a + b : size * a + b + 1, :] = v
    for a, v in enumerate(p + z):
        at = size * size + a
        table[at : at + 1, :] = fold(v * r)
    row[...] = lax.dot_general(
        jnp.ones((8, 128), f32),
        table[...],
        (((1,), (1,)), ((), ())),
        precision=lax.Precision.HIGHEST,
        preferred_element_type=f32,
    )[0:1, :]


def total_kernel(parts, gram, projections, *, scale):
    size = 2 * STEPS + 1
    total = parts[0]
    for n in range(1, parts.shape[0]):
        total = total + parts[n]
    total = total * scale
    wide = jnp.broadcast_to(total, (8, 128))
    for a in range(size):
        v = pltpu.roll(wide, (128 - size * a) % 128, 1) if a else wide
        gram[a : a + 1, :] = v[0:1, 0:size]
    v = pltpu.roll(wide, (128 - size * size) % 128, 1)
    projections[...] = v[0:1, 0:size]


VMEM = pl.BlockSpec(memory_space=pltpu.VMEM)
SMEM = pl.BlockSpec(memory_space=pltpu.SMEM)


def shaped(*dims):
    return jax.ShapeDtypeStruct(dims, f32)


def pack(direction, residual):
    return pl.pallas_call(
        pack_kernel,
        in_specs=[VMEM, VMEM],
        out_specs=[VMEM, VMEM],
        out_shape=[shaped(2, 8, 128), shaped(2, 8, 128)],
        compiler_params=pltpu.CompilerParams(vmem_limit_bytes=2 * 1024 * 1024),
        name="pack",
    )(direction, residual)


def powers_of(where, own, low, high, interpret=False):
    padded = (2, PLANES + 2 * LEAD, ROWS + 2 * PAD, 128)
    plain = (2, PLANES + 2 * LEAD, ROWS, 128)
    return pl.pallas_call(
        powers_kernel,
        in_specs=[SMEM, VMEM, VMEM, VMEM],
        out_specs=[VMEM] * 4,
        out_shape=[
            shaped(STEPS, 8, 8, 128),
            shaped(2 * STEPS + 1, 8, 8, 128),
            shaped(STEPS + 1, 8, 8, 128),
            shaped(16, 128),
        ],
        scratch_shapes=[pltpu.VMEM(padded, f32)] * 5
        + [pltpu.VMEM((STEPS + 1, PLANES + 2 * LEAD, ROWS, 128), f32)]
        + [pltpu.VMEM(plain, f32), pltpu.VMEM(plain, f32), pltpu.VMEM(padded, f32), pltpu.VMEM(padded, f32)]
        + [pltpu.VMEM(plain, f32)] * 3
        + [pltpu.VMEM((2, 7, 8, 128), f32), pltpu.VMEM((4, ROWS, 128), f32)],
        compiler_params=pltpu.CompilerParams(vmem_limit_bytes=44 * 1024 * 1024),
        interpret=interpret,
        name="powers",
    )(where, own, low, high)


def products(where, mine, other, images, sums, direction, residual, interpret=False):
    return pl.pallas_call(
        products_kernel,
        in_specs=[SMEM] + [VMEM] * 6,
        out_specs=[VMEM, VMEM],
        out_shape=[shaped(2, STEPS, 8, 8, 128), shaped(1, 128)],
        scratch_shapes=[pltpu.VMEM((128, 128), f32)],
        interpret=interpret,
        compiler_params=pltpu.CompilerParams(vmem_limit_bytes=2 * 1024 * 1024),
        name="products",
    )(where, mine, other, images, sums, direction, residual)


def totals(parts, scale, interpret=False):
    size = 2 * STEPS + 1

    def kernel(parts_ref, gram, projections):
        total_kernel(parts_ref, gram, projections, scale=scale)

    return pl.pallas_call(
        kernel,
        in_specs=[VMEM],
        out_specs=[VMEM, VMEM],
        out_shape=[shaped(size, size), shaped(1, size)],
        interpret=interpret,
        compiler_params=pltpu.CompilerParams(vmem_limit_bytes=2 * 1024 * 1024),
        name="totals",
    )(parts)


def block_message(cells, left, right):
    return jnp.concatenate([cells, left[None], right[None]], axis=0)


def x_messages(own):
    n = SHORT - 2
    first, second = own[:TILES], own[TILES:]
    flat = lambda v: v.reshape(-1, 8, 128)
    up = jnp.concatenate([flat(first[:, BX - n :]), flat(second)], axis=0)
    short = jnp.concatenate([second[:, :n], second[:, BX:]], axis=1)
    down = jnp.concatenate([flat(first), flat(short)], axis=0)
    return up, down


def forward(n):
    return [(i, i + 1) for i in range(n - 1)]


def backward(n):
    return [(i + 1, i) for i in range(n - 1)]


def everyone(x, axes, count):
    return lax.all_to_all(jnp.broadcast_to(x[None], (count,) + x.shape), axes, 0, 0)


def local(residual, direction):
    nx, ny, nz = lax.axis_size("gx_0"), lax.axis_size("gy"), lax.axis_size("gz")
    iz = lax.axis_index("gz")
    where = jnp.stack(
        [
            lax.axis_index("gx_1"),
            lax.axis_index("gx_0"),
            lax.axis_index("gy"),
            iz,
            jnp.int32(nx * SLAB),
            jnp.where(iz < nz - 1, 1, 0),
        ]
    ).astype(jnp.int32)
    up, down = pack(direction, residual)
    left = lax.ppermute(up, "gz", forward(nz))
    right = lax.ppermute(down, "gz", backward(nz))
    message = jnp.stack(
        [block_message(direction, left[0], right[0]), block_message(residual, left[1], right[1])]
    )
    message = jnp.broadcast_to(message[:, None], (2, TILES) + message.shape[1:])
    own = lax.all_to_all(message.reshape((2 * TILES,) + message.shape[2:]), ("gx_1", "gy"), 0, 0)
    send_up, send_down = x_messages(own)
    low = lax.ppermute(send_up, "gx_0", forward(nx))
    high = lax.ppermute(send_down, "gx_0", backward(nx))
    mine, theirs, images, sums = powers_of(where, own, low, high)
    other = lax.ppermute(theirs, "gx_1", [(0, 1), (1, 0)])
    powers, row = products(where, mine, other, images, sums, direction, residual)
    row = jnp.sum(everyone(row, ("gy", "gz"), ny * nz), axis=0)
    parts = everyone(row, GX, 2 * nx)
    cells = float(2 * nx * BX * ny * BY * nz * BZ)
    gram, projections = totals(parts, 1.0 / cells)
    return powers, gram, projections.reshape(-1)


def solution(mesh):
    torus = Mesh(
        mesh.devices.reshape(mesh.shape["gx"] // 2, 2, mesh.shape["gy"], mesh.shape["gz"]),
        ("gx_0", "gx_1", "gy", "gz"),
    )
    return jax.shard_map(
        local,
        mesh=torus,
        in_specs=(P(GX, "gy", "gz"), P(GX, "gy", "gz")),
        out_specs=(P(None, None, GX, "gy", "gz"), P(), P()),
        check_vma=False,
    )
```

```python
import jax
import jax.numpy as jnp
from jax import lax
from jax.experimental import pallas as pl
from jax.experimental.pallas import tpu as pltpu
from jax.sharding import Mesh
from jax.sharding import PartitionSpec as P

STEPS = 4
GX = ("gx_0", "gx_1")
BX, BY, BZ = 8, 8, 128
SLAB = 2 * BX
HALO = 3 * STEPS + 1
STRIP = 16
TILES = 4
ROWS = TILES * BY
PAD = 8
PLANES = SLAB + 2 * HALO
NB = 10
SHORT = HALO - BX + 2
MSG = TILES * (NB + SHORT)
UNROLL = 4
LEAD = UNROLL + 6
ORIGIN = LEAD + HALO
C0, C1, CS = 117.0, 15.0, 1.0 / 729.0
SUMS = (STEPS + 1) * (STEPS + 2) // 2 + STEPS + 1

f32 = jnp.float32


def lanes():
    return lax.broadcasted_iota(jnp.int32, (8, 128), 1)


def pack_kernel(direction, residual, up, down, buffer, semaphores):
    copies = [
        pltpu.make_async_copy(ref, buffer.at[k], semaphores.at[k])
        for k, ref in enumerate((direction, residual))
    ]
    for copy in copies:
        copy.start()
    for copy in copies:
        copy.wait()
    lane = lanes()
    for k in range(2):
        high = jnp.zeros((8, 128), f32)
        low = jnp.zeros((8, 128), f32)
        for p in range(BX):
            here = (lane >= STRIP * p) & (lane < STRIP * (p + 1))
            v = buffer[k, p]
            high = jnp.where(here, pltpu.roll(v, (STRIP * p - (BZ - STRIP)) % 128, 1), high)
            low = jnp.where(here, pltpu.roll(v, STRIP * p, 1) if p else v, low)
        up[k] = high
        down[k] = low


def powers_kernel(where_ref, own, low, high, residual, slab, theirs, sums, *scratch):
    fields = scratch[:5]
    flat, b_ref, g0_ref, g1_ref, g2_ref, x0_ref, x1_ref, x2_ref, zw, yw = scratch[5:]
    core, ix, iy, iz = where_ref[0], where_ref[1], where_ref[2], where_ref[3]
    lane = lanes()

    one = jnp.ones((8, 128), f32)
    has_l = jnp.where(iz > 0, 1.0, 0.0).astype(f32)
    has_r = where_ref[5].astype(f32)
    first, last = lane == 0, lane == 127
    inside = [one, jnp.where(lane < STRIP, has_r, jnp.where(lane >= 128 - STRIP, has_l, 0.0))]
    for k in range(2):
        if k == 0:
            m = one + jnp.where(first, has_l, 0.0) + jnp.where(last, has_r, 0.0)
            e_left = jnp.where(first, 2.0, 1.0)
            e_right = jnp.where(last, 2.0, 1.0)
            q = jnp.where(first, 2.0 * has_l, 1.0) + jnp.where(last, 2.0 * has_r, 1.0)
        else:
            m = jnp.where(first | last, 2.0, 1.0)
            e_left = jnp.where(first, 2.0, 1.0)
            e_right = jnp.where(last, 2.0, 1.0)
            q = e_left + e_right
        zw[k, 0] = C0 * m + q
        zw[k, 1] = C1 * m
        zw[k, 2] = m
        zw[k, 3] = e_left
        zw[k, 4] = e_right
        zw[k, 5] = inside[k] * CS
        zw[k, 6] = inside[k]

    row = lax.broadcasted_iota(jnp.int32, (ROWS, 128), 0)
    top, bottom = row % BY == 0, row % BY == BY - 1
    e_up = jnp.where(top, 2.0, 1.0)
    e_down = jnp.where(bottom, 2.0, 1.0)
    yw[0] = 1.0 + jnp.where(top & (row > 0), 1.0, 0.0) + jnp.where(bottom & (row < ROWS - 1), 1.0, 0.0)
    yw[1] = e_up
    yw[2] = e_down
    yw[3] = jnp.where(row > 0, e_up, 0.0) + jnp.where(row < ROWS - 1, e_down, 0.0)

    blank = jnp.zeros((PAD, 128), f32)

    def clear(i, _):
        for ref in list(fields) + [g1_ref, g2_ref]:
            for k in range(2):
                ref[k, i, 0:PAD, :] = blank
                ref[k, i, PAD + ROWS : PAD + ROWS + PAD, :] = blank
        return 0

    lax.fori_loop(LEAD, LEAD + PLANES, clear, 0)

    def place(x, t, center, left, right):
        p = x % BX
        rows = slice(PAD + BY * t, PAD + BY * (t + 1))
        fields[0][0, x + ORIGIN, rows, :] = center
        shift_r = (-STRIP * p) % 128
        shift_l = (128 - STRIP - STRIP * p) % 128
        r = pltpu.roll(right, shift_r, 1) if shift_r else right
        l = pltpu.roll(left, shift_l, 1) if shift_l else left
        fields[0][1, x + ORIGIN, rows, :] = jnp.where(
            lane < STRIP, r, jnp.where(lane >= 128 - STRIP, l, 0.0)
        )

    for t in range(TILES):
        for c in range(2):
            left, right = own[TILES * c + t, BX], own[TILES * c + t, BX + 1]
            for p in range(BX):
                place(BX * c + p, t, own[TILES * c + t, p], left, right)
        n = SHORT - 2
        base = SHORT * t
        for p in range(n):
            place(p - HALO, t, low[base + p], low[base + n], low[base + n + 1])
        base = SHORT * TILES + NB * t
        for p in range(BX):
            place(p - BX, t, low[base + p], low[base + BX], low[base + BX + 1])
        base = NB * t
        for p in range(BX):
            place(SLAB + p, t, high[base + p], high[base + BX], high[base + BX + 1])
        base = NB * TILES + SHORT * t
        for p in range(n):
            place(SLAB + BX + p, t, high[base + p], high[base + n], high[base + n + 1])

    lane_row = lax.broadcasted_iota(jnp.int32, (ROWS, 128), 1)

    def left_of(c, s, d):
        rc, rs = pltpu.roll(c, d, 1), pltpu.roll(s, d, 1)
        edge = lane_row < d
        return jnp.where(edge, rs, rc), jnp.where(edge, rc, rs)

    def right_of(c, s, d):
        rc, rs = pltpu.roll(c, 128 - d, 1), pltpu.roll(s, 128 - d, 1)
        edge = lane_row >= 128 - d
        return jnp.where(edge, rs, rc), jnp.where(edge, rc, rs)

    n_planes = where_ref[4]

    def in_grid(i):
        g = ix * SLAB + i - ORIGIN
        return jnp.where((g >= 0) & (g < n_planes), 1.0, 0.0).astype(f32)

    def z_row(k, j):
        return zw[k, j][0:1, :]

    def around(ref, i):
        c, s = ref[0, i, PAD : PAD + ROWS, :], ref[1, i, PAD : PAD + ROWS, :]
        lc, ls = left_of(c, s, 1)
        rc, rs = right_of(c, s, 1)
        out = []
        for k, (v, a, b) in enumerate(((c, lc, rc), (s, ls, rs))):
            n = a + b
            n = n + (ref[k, i, PAD - 1 : PAD - 1 + ROWS, :] + ref[k, i, PAD + 1 : PAD + 1 + ROWS, :])
            n = n + (ref[k, i - 1, PAD : PAD + ROWS, :] + ref[k, i + 1, PAD : PAD + ROWS, :])
            out.append((v, n))
        return out

    for step in range(STEPS):
        source, target = fields[step], fields[step + 1]
        lo_b = LEAD + 1 + 3 * step
        hi_b = LEAD + PLANES - 1 - 3 * step

        def image(i, step=step, source=source):
            (c, nc), (s, ns) = around(source, i)
            if step == 0:
                center = jnp.where(core == 0, 6.0, 1.0).astype(f32)
                beside = jnp.where(core == 0, 1.0, 0.0).astype(f32)
                ac, as_ = center * c - beside * nc, center * s - beside * ns
            else:
                ac, as_ = 6.0 * c - nc, 6.0 * s - ns
            flat[step, i] = ac
            keep = in_grid(i)
            b_ref[0, i] = ac * (z_row(0, 5) * keep)
            b_ref[1, i] = as_ * (z_row(1, 5) * keep)

        def along_z(i):
            bc, bs = b_ref[0, i], b_ref[1, i]
            l1c, l1s = left_of(bc, bs, 1)
            r1c, r1s = right_of(bc, bs, 1)
            l2c, l2s = left_of(bc, bs, 2)
            r2c, r2s = right_of(bc, bs, 2)
            for k, (b, l1, r1, l2, r2) in enumerate(((bc, l1c, r1c, l2c, r2c), (bs, l1s, r1s, l2s, r2s))):
                e = z_row(k, 3) * l1 + z_row(k, 4) * r1
                g0_ref[k, i] = z_row(k, 0) * b + C1 * e + (l2 + r2)
                g1_ref[k, i, PAD : PAD + ROWS, :] = z_row(k, 1) * b + (e + e)
                g2_ref[k, i, PAD : PAD + ROWS, :] = z_row(k, 2) * b


        def along_y(i):
            for k in range(2):
                g1 = g1_ref[k, i, PAD : PAD + ROWS, :]
                g2 = g2_ref[k, i, PAD : PAD + ROWS, :]
                m, up, down, q = yw[0], yw[1], yw[2], yw[3]
                e1 = up * g1_ref[k, i, PAD - 1 : PAD - 1 + ROWS, :] + down * g1_ref[k, i, PAD + 1 : PAD + 1 + ROWS, :]
                e2 = up * g2_ref[k, i, PAD - 1 : PAD - 1 + ROWS, :] + down * g2_ref[k, i, PAD + 1 : PAD + 1 + ROWS, :]
                far = g2_ref[k, i, PAD - 2 : PAD - 2 + ROWS, :] + g2_ref[k, i, PAD + 2 : PAD + 2 + ROWS, :]
                x0_ref[k, i] = m * g0_ref[k, i] + e1 + (q * g2 + far)
                x1_ref[k, i] = m * g1 + (e2 + e2)
                x2_ref[k, i] = m * g2


        def along_x(i, target=target):
            g = ix * SLAB + i - ORIGIN
            keep = in_grid(i)
            p = g & (BX - 1)
            before = jnp.where(p == 0, 2.0, 1.0).astype(f32)
            after = jnp.where(p == BX - 1, 2.0, 1.0).astype(f32)
            some_before = jnp.where(g > 0, 1.0, 0.0).astype(f32)
            some_after = jnp.where(g < n_planes - 1, 1.0, 0.0).astype(f32)
            m = keep * (1.0 + (before - 1.0) * some_before + (after - 1.0) * some_after)
            q = keep * (before * some_before + after * some_after)
            wl, wr = keep * before, keep * after
            for k in range(2):
                v = m * x0_ref[k, i] + q * x2_ref[k, i]
                v = v + (wl * x1_ref[k, i - 1] + wr * x1_ref[k, i + 1])
                v = v + keep * (x2_ref[k, i - 2] + x2_ref[k, i + 2])
                if k == 1:
                    v = v * z_row(1, 6)
                target[k, i, PAD : PAD + ROWS, :] = v

        def ahead(i):
            for u in range(UNROLL):
                image(i + u)

        def behind(i):
            for u in range(UNROLL):
                along_z(i + u)
            for u in range(UNROLL):
                along_y(i + u)
            for u in range(UNROLL):
                along_x(i + u - 2)

        def turn(n, _, lo_b=lo_b):
            behind(lo_b + UNROLL * n)
            ahead(lo_b + UNROLL * (n + 1))
            return 0

        turns = -(-(hi_b - lo_b) // UNROLL)
        ahead(lo_b)
        lax.fori_loop(0, turns - 1, turn, 0)
        behind(lo_b + UNROLL * (turns - 1))

    def last_image(i):
        c, nc = around(fields[STEPS], i)[0]
        flat[STEPS, i] = 6.0 * c - nc

    def last_turn(n, _):
        for u in range(SLAB // 2):
            last_image(ORIGIN + SLAB // 2 * n + u)
        return 0

    lax.fori_loop(0, 2, last_turn, 0)

    rows = pl.ds(pl.multiple_of(PAD + BY * iy, 8), BY)
    for j in range(STEPS):
        slab[j] = fields[j + 1][0, ORIGIN : ORIGIN + SLAB, PAD : PAD + ROWS, :]
        theirs[BX * j : BX * (j + 1)] = fields[j + 1][0, pl.ds(ORIGIN + BX * (1 - core), BX), rows, :]
    for x in range(SLAB):
        for t in range(TILES):
            theirs[BX * STEPS + TILES * x + t] = flat[STEPS, ORIGIN + x, BY * t : BY * (t + 1), :]

    pairs = [(a, b) for a in range(STEPS + 1) for b in range(a, STEPS + 1)]

    def add_plane(x, carry):
        i = ORIGIN + x
        carry = list(carry)
        for t in range(TILES):
            fs = [fields[j][0, i, PAD + BY * t : PAD + BY * (t + 1), :] for j in range(STEPS + 1)]
            im = [flat[j, i, BY * t : BY * (t + 1), :] for j in range(STEPS + 1)]
            r = jnp.where(core == 0, residual[x, t], fs[0])
            for n, (a, b) in enumerate(pairs):
                carry[n] = carry[n] + fs[a] * im[b]
            for a in range(STEPS + 1):
                carry[len(pairs) + a] = carry[len(pairs) + a] + fs[a] * r
        return tuple(carry)

    totals = lax.fori_loop(0, SLAB, add_plane, tuple(jnp.zeros((8, 128), f32) for _ in range(SUMS)))
    sums[...] = jnp.zeros((24, 128), f32)
    for n, total in enumerate(totals):
        sums[n : n + 1, :] = jnp.sum(total, axis=0, keepdims=True)


def products_kernel(where_ref, slab, other, sums, powers, row, table):
    north = where_ref[0] == 0
    core, iy = where_ref[0], where_ref[2]
    rows = pl.ds(pl.multiple_of(BY * iy, 8), BY)
    for j in range(STEPS):
        own = slab[j, pl.ds(BX * core, BX), rows, :]
        far = other[BX * j : BX * (j + 1)]
        powers[0, j] = jnp.where(north, own, far)
        powers[1, j] = jnp.where(north, far, own)

    def add_plane(x, carry):
        carry = list(carry)
        for t in range(TILES):
            image = other[BX * STEPS + TILES * x + t]
            for j in range(STEPS):
                carry[j] = carry[j] + slab[j, x, BY * t : BY * (t + 1), :] * image
        return tuple(carry)

    cross = lax.fori_loop(0, SLAB, add_plane, tuple(jnp.zeros((8, 128), f32) for _ in range(STEPS)))
    cross = [jnp.sum(v, axis=0, keepdims=True) for v in cross]

    zero = jnp.zeros((1, 128), f32)
    local = {}
    n = 0
    for a in range(STEPS + 1):
        for b in range(a, STEPS + 1):
            local[a, b] = local[b, a] = sums[n : n + 1, :]
            n += 1
    against = [sums[n + a : n + a + 1, :] for a in range(STEPS + 1)]
    hankel = against[1:] + cross
    table[...] = jnp.zeros((128, 128), f32)
    size = 2 * STEPS + 1
    for a in range(size):
        for b in range(size):
            if a > STEPS and b > STEPS:
                v = jnp.where(north, zero, local[a - STEPS, b - STEPS])
            elif a <= STEPS and b <= STEPS:
                v = jnp.where(north, local[a, b], zero)
            else:
                v = jnp.where(north, hankel[a + b - STEPS - 1], zero)
            table[size * a + b : size * a + b + 1, :] = v
    for a in range(STEPS + 1):
        table[size * size + a : size * size + a + 1, :] = jnp.where(north, against[a], zero)
        if a:
            at = size * size + STEPS + a
            table[at : at + 1, :] = jnp.where(north, zero, against[a])
    row[...] = lax.dot_general(
        jnp.ones((8, 128), f32),
        table[...],
        (((1,), (1,)), ((), ())),
        precision=lax.Precision.HIGHEST,
        preferred_element_type=f32,
    )[0:1, :]


def total_kernel(parts, gram, projections, *, scale):
    size = 2 * STEPS + 1
    total = parts[0]
    for n in range(1, parts.shape[0]):
        total = total + parts[n]
    total = total * scale
    wide = jnp.broadcast_to(total, (8, 128))
    for a in range(size):
        v = pltpu.roll(wide, (128 - size * a) % 128, 1) if a else wide
        gram[a : a + 1, :] = v[0:1, 0:size]
    v = pltpu.roll(wide, (128 - size * size) % 128, 1)
    projections[...] = v[0:1, 0:size]


VMEM = pl.BlockSpec(memory_space=pltpu.VMEM)
SMEM = pl.BlockSpec(memory_space=pltpu.SMEM)


def shaped(*dims):
    return jax.ShapeDtypeStruct(dims, f32)


def pack(direction, residual):
    return pl.pallas_call(
        pack_kernel,
        in_specs=[pl.BlockSpec(memory_space=pltpu.HBM)] * 2,
        out_specs=[VMEM, VMEM],
        out_shape=[shaped(2, 8, 128), shaped(2, 8, 128)],
        scratch_shapes=[pltpu.VMEM((2, BX, 8, 128), f32), pltpu.SemaphoreType.DMA((2,))],
        compiler_params=pltpu.CompilerParams(vmem_limit_bytes=2 * 1024 * 1024),
        name="pack",
    )(direction, residual)


def powers_of(where, own, low, high, residual, interpret=False):
    padded = (2, PLANES + 2 * LEAD, ROWS + 2 * PAD, 128)
    plain = (2, PLANES + 2 * LEAD, ROWS, 128)
    return pl.pallas_call(
        powers_kernel,
        in_specs=[SMEM, VMEM, VMEM, VMEM, VMEM],
        out_specs=[VMEM] * 3,
        out_shape=[
            shaped(STEPS, SLAB, ROWS, 128),
            shaped(BX * STEPS + TILES * SLAB, 8, 128),
            shaped(24, 128),
        ],
        scratch_shapes=[pltpu.VMEM(padded, f32)] * 5
        + [pltpu.VMEM((STEPS + 1, PLANES + 2 * LEAD, ROWS, 128), f32)]
        + [pltpu.VMEM(plain, f32), pltpu.VMEM(plain, f32), pltpu.VMEM(padded, f32), pltpu.VMEM(padded, f32)]
        + [pltpu.VMEM(plain, f32)] * 3
        + [pltpu.VMEM((2, 7, 8, 128), f32), pltpu.VMEM((4, ROWS, 128), f32)],
        compiler_params=pltpu.CompilerParams(vmem_limit_bytes=44 * 1024 * 1024),
        interpret=interpret,
        name="powers",
    )(where, own, low, high, residual)


def products(where, slab, other, sums, interpret=False):
    return pl.pallas_call(
        products_kernel,
        in_specs=[SMEM] + [VMEM] * 3,
        out_specs=[VMEM, VMEM],
        out_shape=[shaped(2, STEPS, 8, 8, 128), shaped(1, 128)],
        scratch_shapes=[pltpu.VMEM((128, 128), f32)],
        interpret=interpret,
        compiler_params=pltpu.CompilerParams(vmem_limit_bytes=4 * 1024 * 1024),
        name="products",
    )(where, slab, other, sums)


def totals(parts, scale, interpret=False):
    size = 2 * STEPS + 1

    def kernel(parts_ref, gram, projections):
        total_kernel(parts_ref, gram, projections, scale=scale)

    return pl.pallas_call(
        kernel,
        in_specs=[VMEM],
        out_specs=[VMEM, VMEM],
        out_shape=[shaped(size, size), shaped(1, size)],
        interpret=interpret,
        compiler_params=pltpu.CompilerParams(vmem_limit_bytes=2 * 1024 * 1024),
        name="totals",
    )(parts)


def block_message(cells, left, right):
    return jnp.concatenate([cells, left[None], right[None]], axis=0)


def x_messages(own):
    n = SHORT - 2
    first, second = own[:TILES], own[TILES:]
    flat = lambda v: v.reshape(-1, 8, 128)
    up = jnp.concatenate([flat(first[:, BX - n :]), flat(second)], axis=0)
    short = jnp.concatenate([second[:, :n], second[:, BX:]], axis=1)
    down = jnp.concatenate([flat(first), flat(short)], axis=0)
    return up, down


def forward(n):
    return [(i, i + 1) for i in range(n - 1)]


def backward(n):
    return [(i + 1, i) for i in range(n - 1)]


def everyone(x, axes, count):
    return lax.all_to_all(jnp.broadcast_to(x[None], (count,) + x.shape), axes, 0, 0)


def local(residual, direction):
    nx, ny, nz = lax.axis_size("gx_0"), lax.axis_size("gy"), lax.axis_size("gz")
    iz = lax.axis_index("gz")
    where = jnp.stack(
        [
            lax.axis_index("gx_1"),
            lax.axis_index("gx_0"),
            lax.axis_index("gy"),
            iz,
            jnp.int32(nx * SLAB),
            jnp.where(iz < nz - 1, 1, 0),
        ]
    ).astype(jnp.int32)
    up, down = pack(direction, residual)
    left = lax.ppermute(up, "gz", forward(nz))
    right = lax.ppermute(down, "gz", backward(nz))
    message = jnp.stack(
        [block_message(direction, left[0], right[0]), block_message(residual, left[1], right[1])]
    )
    message = jnp.broadcast_to(message[:, None], (2, TILES) + message.shape[1:])
    own = lax.all_to_all(message.reshape((2 * TILES,) + message.shape[2:]), ("gx_1", "gy"), 0, 0)
    send_up, send_down = x_messages(own)
    low = lax.ppermute(send_up, "gx_0", forward(nx))
    high = lax.ppermute(send_down, "gx_0", backward(nx))
    blocks = own[:, :BX].reshape(2, TILES, BX, 8, 128).swapaxes(1, 2).reshape(SLAB, TILES, 8, 128)
    across = lax.ppermute(blocks, "gx_1", [(1, 0)])
    slab, theirs, sums = powers_of(where, own, low, high, across)
    other = lax.ppermute(theirs, "gx_1", [(0, 1), (1, 0)])
    powers, row = products(where, slab, other, sums)
    row = jnp.sum(everyone(row, ("gx_1", "gz"), 2 * nz), axis=0)
    parts = everyone(row, "gx_0", nx)
    cells = float(2 * nx * BX * ny * BY * nz * BZ)
    gram, projections = totals(parts, 1.0 / cells)
    return powers, gram, projections.reshape(-1)


def solution(mesh):
    torus = Mesh(
        mesh.devices.reshape(mesh.shape["gx"] // 2, 2, mesh.shape["gy"], mesh.shape["gz"]),
        ("gx_0", "gx_1", "gy", "gz"),
    )
    return jax.shard_map(
        local,
        mesh=torus,
        in_specs=(P(GX, "gy", "gz"), P(GX, "gy", "gz")),
        out_specs=(P(None, None, GX, "gy", "gz"), P(), P()),
        check_vma=False,
    )
```

```python
import jax
import jax.numpy as jnp
from jax import lax
from jax.experimental import pallas as pl
from jax.experimental.pallas import tpu as pltpu
from jax.sharding import Mesh
from jax.sharding import PartitionSpec as P

STEPS = 4
GX = ("gx_0", "gx_1")
BX, BY, BZ = 8, 8, 128
SLAB = 2 * BX
HALO = 3 * STEPS + 1
STRIP = 16
TILES = 4
ROWS = TILES * BY
PAD = 8
PLANES = SLAB + 2 * HALO
NB = 10
SHORT = HALO - BX + 1
MSG = TILES * (NB + SHORT)
TURN = (10, 12, 14, 11)
LEAD = 6
ORIGIN = LEAD + HALO
C0, C1, CS = 117.0, 15.0, 1.0 / 729.0
SUMS = (STEPS + 1) * (STEPS + 2) // 2 + STEPS + 1

f32 = jnp.float32


def lanes():
    return lax.broadcasted_iota(jnp.int32, (8, 128), 1)


def pack_kernel(direction, residual, up, down, buffer, semaphores):
    copies = [
        pltpu.make_async_copy(ref, buffer.at[k], semaphores.at[k])
        for k, ref in enumerate((direction, residual))
    ]
    for copy in copies:
        copy.start()
    for copy in copies:
        copy.wait()
    lane = lanes()
    for k in range(2):
        high = jnp.zeros((8, 128), f32)
        low = jnp.zeros((8, 128), f32)
        for p in range(BX):
            here = (lane >= STRIP * p) & (lane < STRIP * (p + 1))
            v = buffer[k, p]
            high = jnp.where(here, pltpu.roll(v, (STRIP * p - (BZ - STRIP)) % 128, 1), high)
            low = jnp.where(here, pltpu.roll(v, STRIP * p, 1) if p else v, low)
        up[k] = high
        down[k] = low


def powers_kernel(where_ref, own, low, high, residual, slab, theirs, sums, *scratch):
    fields = scratch[:5]
    flat, b_ref, g0_ref, g1_ref, g2_ref, x0_ref, x1_ref, x2_ref, zw, yw = scratch[5:]
    core, ix, iy, iz = where_ref[0], where_ref[1], where_ref[2], where_ref[3]
    lane = lanes()

    one = jnp.ones((8, 128), f32)
    has_l = jnp.where(iz > 0, 1.0, 0.0).astype(f32)
    has_r = where_ref[5].astype(f32)
    first, last = lane == 0, lane == 127
    inside = [one, jnp.where(lane < STRIP, has_r, jnp.where(lane >= 128 - STRIP, has_l, 0.0))]
    for k in range(2):
        if k == 0:
            m = one + jnp.where(first, has_l, 0.0) + jnp.where(last, has_r, 0.0)
            e_left = jnp.where(first, 2.0, 1.0)
            e_right = jnp.where(last, 2.0, 1.0)
            q = jnp.where(first, 2.0 * has_l, 1.0) + jnp.where(last, 2.0 * has_r, 1.0)
        else:
            m = jnp.where(first | last, 2.0, 1.0)
            e_left = jnp.where(first, 2.0, 1.0)
            e_right = jnp.where(last, 2.0, 1.0)
            q = e_left + e_right
        zw[k, 0] = C0 * m + q
        zw[k, 1] = C1 * m
        zw[k, 2] = m
        zw[k, 3] = e_left
        zw[k, 4] = e_right
        zw[k, 5] = inside[k] * CS
        zw[k, 6] = inside[k]

    row = lax.broadcasted_iota(jnp.int32, (ROWS, 128), 0)
    top, bottom = row % BY == 0, row % BY == BY - 1
    e_up = jnp.where(top, 2.0, 1.0)
    e_down = jnp.where(bottom, 2.0, 1.0)
    yw[0] = 1.0 + jnp.where(top & (row > 0), 1.0, 0.0) + jnp.where(bottom & (row < ROWS - 1), 1.0, 0.0)
    yw[1] = e_up
    yw[2] = e_down
    yw[3] = jnp.where(row > 0, e_up, 0.0) + jnp.where(row < ROWS - 1, e_down, 0.0)

    blank = jnp.zeros((PAD, 128), f32)

    def clear(i, _):
        for ref in list(fields) + [g1_ref, g2_ref]:
            for k in range(2):
                ref[k, i, 0:PAD, :] = blank
                ref[k, i, PAD + ROWS : PAD + ROWS + PAD, :] = blank
        return 0

    lax.fori_loop(LEAD, LEAD + PLANES, clear, 0)

    def place(x, t, center, left, right):
        p = x % BX
        rows = slice(PAD + BY * t, PAD + BY * (t + 1))
        fields[0][0, x + ORIGIN, rows, :] = center
        shift_r = (-STRIP * p) % 128
        shift_l = (128 - STRIP - STRIP * p) % 128
        r = pltpu.roll(right, shift_r, 1) if shift_r else right
        l = pltpu.roll(left, shift_l, 1) if shift_l else left
        fields[0][1, x + ORIGIN, rows, :] = jnp.where(
            lane < STRIP, r, jnp.where(lane >= 128 - STRIP, l, 0.0)
        )

    for t in range(TILES):
        for c in range(2):
            left, right = own[TILES * c + t, BX], own[TILES * c + t, BX + 1]
            for p in range(BX):
                place(BX * c + p, t, own[TILES * c + t, p], left, right)
        n = SHORT - 1
        base = SHORT * t
        for p in range(n):
            place(p - HALO, t, low[base + p], low[base + n], low[base + n])
        base = SHORT * TILES + NB * t
        for p in range(BX):
            place(p - BX, t, low[base + p], low[base + BX], low[base + BX + 1])
        base = NB * t
        for p in range(BX):
            place(SLAB + p, t, high[base + p], high[base + BX], high[base + BX + 1])
        base = NB * TILES + SHORT * t
        for p in range(n):
            place(SLAB + BX + p, t, high[base + p], high[base + n], high[base + n])

    lane_row = lax.broadcasted_iota(jnp.int32, (ROWS, 128), 1)

    def left_of(c, s, d):
        rc, rs = pltpu.roll(c, d, 1), pltpu.roll(s, d, 1)
        edge = lane_row < d
        return jnp.where(edge, rs, rc), jnp.where(edge, rc, rs)

    def right_of(c, s, d):
        rc, rs = pltpu.roll(c, 128 - d, 1), pltpu.roll(s, 128 - d, 1)
        edge = lane_row >= 128 - d
        return jnp.where(edge, rs, rc), jnp.where(edge, rc, rs)

    n_planes = where_ref[4]

    def in_grid(i):
        g = ix * SLAB + i - ORIGIN
        return jnp.where((g >= 0) & (g < n_planes), 1.0, 0.0).astype(f32)

    def z_row(k, j):
        return zw[k, j][0:1, :]

    def around(ref, i):
        c, s = ref[0, i, PAD : PAD + ROWS, :], ref[1, i, PAD : PAD + ROWS, :]
        lc, ls = left_of(c, s, 1)
        rc, rs = right_of(c, s, 1)
        out = []
        for k, (v, a, b) in enumerate(((c, lc, rc), (s, ls, rs))):
            n = a + b
            n = n + (ref[k, i, PAD - 1 : PAD - 1 + ROWS, :] + ref[k, i, PAD + 1 : PAD + 1 + ROWS, :])
            n = n + (ref[k, i - 1, PAD : PAD + ROWS, :] + ref[k, i + 1, PAD : PAD + ROWS, :])
            out.append((v, n))
        return out

    for step in range(STEPS):
        source, target = fields[step], fields[step + 1]
        lo_b = LEAD + 1 + 3 * step
        hi_b = LEAD + PLANES - 1 - 3 * step

        def image(i, step=step, source=source):
            (c, nc), (s, ns) = around(source, i)
            if step == 0:
                center = jnp.where(core == 0, 6.0, 1.0).astype(f32)
                beside = jnp.where(core == 0, 1.0, 0.0).astype(f32)
                ac, as_ = center * c - beside * nc, center * s - beside * ns
            else:
                ac, as_ = 6.0 * c - nc, 6.0 * s - ns
            flat[step, i] = ac
            keep = in_grid(i)
            b_ref[0, i] = ac * (z_row(0, 5) * keep)
            b_ref[1, i] = as_ * (z_row(1, 5) * keep)

        def along_z(i):
            bc, bs = b_ref[0, i], b_ref[1, i]
            l1c, l1s = left_of(bc, bs, 1)
            r1c, r1s = right_of(bc, bs, 1)
            l2c, l2s = left_of(bc, bs, 2)
            r2c, r2s = right_of(bc, bs, 2)
            for k, (b, l1, r1, l2, r2) in enumerate(((bc, l1c, r1c, l2c, r2c), (bs, l1s, r1s, l2s, r2s))):
                e = z_row(k, 3) * l1 + z_row(k, 4) * r1
                g0_ref[k, i] = z_row(k, 0) * b + C1 * e + (l2 + r2)
                g1_ref[k, i, PAD : PAD + ROWS, :] = z_row(k, 1) * b + (e + e)
                g2_ref[k, i, PAD : PAD + ROWS, :] = z_row(k, 2) * b


        def along_y(i):
            for k in range(2):
                g1 = g1_ref[k, i, PAD : PAD + ROWS, :]
                g2 = g2_ref[k, i, PAD : PAD + ROWS, :]
                m, up, down, q = yw[0], yw[1], yw[2], yw[3]
                e1 = up * g1_ref[k, i, PAD - 1 : PAD - 1 + ROWS, :] + down * g1_ref[k, i, PAD + 1 : PAD + 1 + ROWS, :]
                e2 = up * g2_ref[k, i, PAD - 1 : PAD - 1 + ROWS, :] + down * g2_ref[k, i, PAD + 1 : PAD + 1 + ROWS, :]
                far = g2_ref[k, i, PAD - 2 : PAD - 2 + ROWS, :] + g2_ref[k, i, PAD + 2 : PAD + 2 + ROWS, :]
                x0_ref[k, i] = m * g0_ref[k, i] + e1 + (q * g2 + far)
                x1_ref[k, i] = m * g1 + (e2 + e2)
                x2_ref[k, i] = m * g2


        def along_x(i, target=target):
            g = ix * SLAB + i - ORIGIN
            keep = in_grid(i)
            p = g & (BX - 1)
            before = jnp.where(p == 0, 2.0, 1.0).astype(f32)
            after = jnp.where(p == BX - 1, 2.0, 1.0).astype(f32)
            some_before = jnp.where(g > 0, 1.0, 0.0).astype(f32)
            some_after = jnp.where(g < n_planes - 1, 1.0, 0.0).astype(f32)
            m = keep * (1.0 + (before - 1.0) * some_before + (after - 1.0) * some_after)
            q = keep * (before * some_before + after * some_after)
            wl, wr = keep * before, keep * after
            for k in range(2):
                v = m * x0_ref[k, i] + q * x2_ref[k, i]
                v = v + (wl * x1_ref[k, i - 1] + wr * x1_ref[k, i + 1])
                v = v + keep * (x2_ref[k, i - 2] + x2_ref[k, i + 2])
                if k == 1:
                    v = v * z_row(1, 6)
                target[k, i, PAD : PAD + ROWS, :] = v

        count = TURN[step]

        def turn(n, _, lo_b=lo_b, count=count):
            i = lo_b + count * n
            for u in range(count):
                image(i + u)
            for u in range(count):
                along_z(i + u)
            for u in range(count):
                along_y(i + u)
            for u in range(count):
                along_x(i + u - 2)
            return 0

        lax.fori_loop(0, -(-(hi_b - lo_b) // count), turn, 0)

    def last_image(i):
        c, nc = around(fields[STEPS], i)[0]
        flat[STEPS, i] = 6.0 * c - nc

    def last_turn(n, _):
        for u in range(SLAB // 2):
            last_image(ORIGIN + SLAB // 2 * n + u)
        return 0

    lax.fori_loop(0, 2, last_turn, 0)

    rows = pl.ds(pl.multiple_of(PAD + BY * iy, 8), BY)
    for j in range(STEPS):
        slab[j] = fields[j + 1][0, ORIGIN : ORIGIN + SLAB, PAD : PAD + ROWS, :]
        theirs[BX * j : BX * (j + 1)] = fields[j + 1][0, pl.ds(ORIGIN + BX * (1 - core), BX), rows, :]
    for x in range(SLAB):
        for t in range(TILES):
            theirs[BX * STEPS + TILES * x + t] = flat[STEPS, ORIGIN + x, BY * t : BY * (t + 1), :]

    pairs = [(a, b) for a in range(STEPS + 1) for b in range(a, STEPS + 1)]

    def add_plane(x, carry):
        i = ORIGIN + x
        carry = list(carry)
        for t in range(TILES):
            fs = [fields[j][0, i, PAD + BY * t : PAD + BY * (t + 1), :] for j in range(STEPS + 1)]
            im = [flat[j, i, BY * t : BY * (t + 1), :] for j in range(STEPS + 1)]
            r = jnp.where(core == 0, residual[x, t], fs[0])
            for n, (a, b) in enumerate(pairs):
                carry[n] = carry[n] + fs[a] * im[b]
            for a in range(STEPS + 1):
                carry[len(pairs) + a] = carry[len(pairs) + a] + fs[a] * r
        return tuple(carry)

    totals = lax.fori_loop(0, SLAB, add_plane, tuple(jnp.zeros((8, 128), f32) for _ in range(SUMS)))
    sums[...] = jnp.zeros((24, 128), f32)
    for n, total in enumerate(totals):
        sums[n : n + 1, :] = jnp.sum(total, axis=0, keepdims=True)


def products_kernel(where_ref, slab, other, sums, powers, row, table, semaphores):
    north = where_ref[0] == 0
    core, iy = where_ref[0], where_ref[2]
    rows = pl.ds(pl.multiple_of(BY * iy, 8), BY)
    copies = [
        pltpu.make_async_copy(slab.at[:, pl.ds(BX * core, BX), rows, :], powers.at[core], semaphores.at[STEPS])
    ]
    for j in range(STEPS):
        copies.append(
            pltpu.make_async_copy(other.at[BX * j : BX * (j + 1)], powers.at[1 - core, j], semaphores.at[j])
        )
    for copy in copies:
        copy.start()

    def add_plane(x, carry):
        carry = list(carry)
        for t in range(TILES):
            image = other[BX * STEPS + TILES * x + t]
            for j in range(STEPS):
                carry[j] = carry[j] + slab[j, x, BY * t : BY * (t + 1), :] * image
        return tuple(carry)

    cross = lax.fori_loop(0, SLAB, add_plane, tuple(jnp.zeros((8, 128), f32) for _ in range(STEPS)))
    cross = [jnp.sum(v, axis=0, keepdims=True) for v in cross]

    zero = jnp.zeros((1, 128), f32)
    local = {}
    n = 0
    for a in range(STEPS + 1):
        for b in range(a, STEPS + 1):
            local[a, b] = local[b, a] = sums[n : n + 1, :]
            n += 1
    against = [sums[n + a : n + a + 1, :] for a in range(STEPS + 1)]
    hankel = against[1:] + cross
    table[...] = jnp.zeros((128, 128), f32)
    size = 2 * STEPS + 1
    for a in range(size):
        for b in range(size):
            if a > STEPS and b > STEPS:
                v = jnp.where(north, zero, local[a - STEPS, b - STEPS])
            elif a <= STEPS and b <= STEPS:
                v = jnp.where(north, local[a, b], zero)
            else:
                v = jnp.where(north, hankel[a + b - STEPS - 1], zero)
            table[size * a + b : size * a + b + 1, :] = v
    for a in range(STEPS + 1):
        table[size * size + a : size * size + a + 1, :] = jnp.where(north, against[a], zero)
        if a:
            at = size * size + STEPS + a
            table[at : at + 1, :] = jnp.where(north, zero, against[a])
    row[...] = lax.dot_general(
        jnp.ones((8, 128), f32),
        table[...],
        (((1,), (1,)), ((), ())),
        precision=lax.Precision.HIGHEST,
        preferred_element_type=f32,
    )[0:1, :]
    for copy in copies:
        copy.wait()


def total_kernel(parts, gram, projections, *, scale):
    size = 2 * STEPS + 1
    total = parts[0]
    for n in range(1, parts.shape[0]):
        total = total + parts[n]
    total = total * scale
    wide = jnp.broadcast_to(total, (8, 128))
    for a in range(size):
        v = pltpu.roll(wide, (128 - size * a) % 128, 1) if a else wide
        gram[a : a + 1, :] = v[0:1, 0:size]
    v = pltpu.roll(wide, (128 - size * size) % 128, 1)
    projections[...] = v[0:1, 0:size]


VMEM = pl.BlockSpec(memory_space=pltpu.VMEM)
SMEM = pl.BlockSpec(memory_space=pltpu.SMEM)


def shaped(*dims):
    return jax.ShapeDtypeStruct(dims, f32)


def pack(direction, residual):
    return pl.pallas_call(
        pack_kernel,
        in_specs=[pl.BlockSpec(memory_space=pltpu.HBM)] * 2,
        out_specs=[VMEM, VMEM],
        out_shape=[shaped(2, 8, 128), shaped(2, 8, 128)],
        scratch_shapes=[pltpu.VMEM((2, BX, 8, 128), f32), pltpu.SemaphoreType.DMA((2,))],
        compiler_params=pltpu.CompilerParams(vmem_limit_bytes=2 * 1024 * 1024),
        name="pack",
    )(direction, residual)


def powers_of(where, own, low, high, residual, interpret=False):
    padded = (2, PLANES + 2 * LEAD, ROWS + 2 * PAD, 128)
    plain = (2, PLANES + 2 * LEAD, ROWS, 128)
    return pl.pallas_call(
        powers_kernel,
        in_specs=[SMEM, VMEM, VMEM, VMEM, VMEM],
        out_specs=[VMEM] * 3,
        out_shape=[
            shaped(STEPS, SLAB, ROWS, 128),
            shaped(BX * STEPS + TILES * SLAB, 8, 128),
            shaped(24, 128),
        ],
        scratch_shapes=[pltpu.VMEM(padded, f32)] * 5
        + [pltpu.VMEM((STEPS + 1, PLANES + 2 * LEAD, ROWS, 128), f32)]
        + [pltpu.VMEM(plain, f32), pltpu.VMEM(plain, f32), pltpu.VMEM(padded, f32), pltpu.VMEM(padded, f32)]
        + [pltpu.VMEM(plain, f32)] * 3
        + [pltpu.VMEM((2, 7, 8, 128), f32), pltpu.VMEM((4, ROWS, 128), f32)],
        compiler_params=pltpu.CompilerParams(vmem_limit_bytes=44 * 1024 * 1024),
        interpret=interpret,
        name="powers",
    )(where, own, low, high, residual)


def products(where, slab, other, sums, interpret=False):
    return pl.pallas_call(
        products_kernel,
        in_specs=[SMEM] + [VMEM] * 3,
        out_specs=[pl.BlockSpec(memory_space=pltpu.HBM), VMEM],
        out_shape=[shaped(2, STEPS, BX, 8, 128), shaped(1, 128)],
        scratch_shapes=[pltpu.VMEM((128, 128), f32), pltpu.SemaphoreType.DMA((STEPS + 1,))],
        interpret=interpret,
        compiler_params=pltpu.CompilerParams(vmem_limit_bytes=4 * 1024 * 1024),
        name="products",
    )(where, slab, other, sums)


def totals(parts, scale, interpret=False):
    size = 2 * STEPS + 1

    def kernel(parts_ref, gram, projections):
        total_kernel(parts_ref, gram, projections, scale=scale)

    return pl.pallas_call(
        kernel,
        in_specs=[VMEM],
        out_specs=[VMEM, VMEM],
        out_shape=[shaped(size, size), shaped(1, size)],
        interpret=interpret,
        compiler_params=pltpu.CompilerParams(vmem_limit_bytes=2 * 1024 * 1024),
        name="totals",
    )(parts)


def block_message(cells, left, right):
    return jnp.concatenate([cells, left[None], right[None]], axis=0)


def messages_kernel(own, up, down, blocks):
    n = SHORT - 1
    low_half = lanes() % STRIP < STRIP // 2
    for t in range(TILES):
        first, second = own.at[t], own.at[TILES + t]
        far = SHORT * t
        up[far : far + n] = first[BX - n : BX]
        up[far + n] = jnp.where(low_half, first[BX + 1], first[BX])
        near = TILES * SHORT + NB * t
        up[near : near + NB] = second[...]
        near = NB * t
        down[near : near + NB] = first[...]
        far = TILES * NB + SHORT * t
        down[far : far + n] = second[0:n]
        down[far + n] = jnp.where(low_half, second[BX + 1], second[BX])
        for p in range(BX):
            blocks[p, t] = first[p]
            blocks[BX + p, t] = second[p]


def x_messages(own, interpret=False):
    return pl.pallas_call(
        messages_kernel,
        in_specs=[VMEM],
        out_specs=[VMEM] * 3,
        out_shape=[shaped(MSG, 8, 128), shaped(MSG, 8, 128), shaped(SLAB, TILES, 8, 128)],
        compiler_params=pltpu.CompilerParams(vmem_limit_bytes=2 * 1024 * 1024),
        interpret=interpret,
        name="messages",
    )(own)


def forward(n):
    return [(i, i + 1) for i in range(n - 1)]


def backward(n):
    return [(i + 1, i) for i in range(n - 1)]


def everyone(x, axes, count):
    return lax.all_to_all(jnp.broadcast_to(x[None], (count,) + x.shape), axes, 0, 0)


def local(residual, direction):
    nx, ny, nz = lax.axis_size("gx_0"), lax.axis_size("gy"), lax.axis_size("gz")
    iz = lax.axis_index("gz")
    where = jnp.stack(
        [
            lax.axis_index("gx_1"),
            lax.axis_index("gx_0"),
            lax.axis_index("gy"),
            iz,
            jnp.int32(nx * SLAB),
            jnp.where(iz < nz - 1, 1, 0),
        ]
    ).astype(jnp.int32)
    up, down = pack(
        pltpu.with_memory_space_constraint(direction, pltpu.HBM),
        pltpu.with_memory_space_constraint(residual, pltpu.HBM),
    )
    left = lax.ppermute(up, "gz", forward(nz))
    right = lax.ppermute(down, "gz", backward(nz))
    message = jnp.stack(
        [block_message(direction, left[0], right[0]), block_message(residual, left[1], right[1])]
    )
    message = jnp.broadcast_to(message[:, None], (2, TILES) + message.shape[1:])
    own = lax.all_to_all(message.reshape((2 * TILES,) + message.shape[2:]), ("gx_1", "gy"), 0, 0)
    send_up, send_down, blocks = x_messages(own)
    low = lax.ppermute(send_up, "gx_0", forward(nx))
    high = lax.ppermute(send_down, "gx_0", backward(nx))
    across = lax.ppermute(blocks, "gx_1", [(1, 0)])
    slab, theirs, sums = powers_of(where, own, low, high, across)
    other = lax.ppermute(theirs, "gx_1", [(0, 1), (1, 0)])
    powers, row = products(where, slab, other, sums)
    row = jnp.sum(everyone(row, ("gx_1", "gz"), 2 * nz), axis=0)
    parts = everyone(row, "gx_0", nx)
    cells = float(2 * nx * BX * ny * BY * nz * BZ)
    gram, projections = totals(parts, 1.0 / cells)
    return powers, gram, projections.reshape(-1)


def solution(mesh):
    torus = Mesh(
        mesh.devices.reshape(mesh.shape["gx"] // 2, 2, mesh.shape["gy"], mesh.shape["gz"]),
        ("gx_0", "gx_1", "gy", "gz"),
    )
    return jax.shard_map(
        local,
        mesh=torus,
        in_specs=(P(GX, "gy", "gz"), P(GX, "gy", "gz")),
        out_specs=(P(None, None, GX, "gy", "gz"), P(), P()),
        check_vma=False,
    )
```
